32 devices in a mesh: gz: 8 (over z, y), ga: 4 (over x, core).
Axes of the slice: x: 2, y: 2, z: 4, core: 2. Of those that a mesh axis runs over, the one named last changes fastest.
Arguments:
- solution: float32 [64, 256, 256], P(('gz', 'ga')), may hold values from -6 to 6
- residual: float32 [64, 256, 256], P(('gz', 'ga')), may hold values from -40 to 40
- direction: float32 [64, 256, 256], P(('gz', 'ga')), may hold values from -40 to 40
Outputs:
- solution_out: float32 [64, 256, 256], P(('gz', 'ga'))
- residual_out: float32 [64, 256, 256], P(('gz', 'ga'))
- direction_out: float32 [64, 256, 256], P(('gz', 'ga'))
The draws below stay inside these ranges and needn't reach their ends.
All inputs are finite; a program needn't handle non-finite values.
Results may differ from the reference program's by a relative error of at most 0.0003.
Values sent between devices are 32-bit elements; how exact they have to be, the bound alone decides.
A program may use at most 128 MiB of HBM per device.

```python
import math
import jax
import jax.numpy as jnp
import numpy as np
from jax import lax

NX = 256
NY = 256
S = 8
NZ = 64


def base_noise(key):
    return jnp.clip(jax.random.normal(key, (NZ, NX, NY), jnp.float32), -3.0, 3.0)


def box_filter(field):
    padded = jnp.pad(field, ((0, 0), (1, 1), (1, 1)))
    total = jnp.zeros_like(field)
    for shift_x in range(3):
        for shift_y in range(3):
            total = total + padded[:, shift_x:shift_x + NX, shift_y:shift_y + NY]
    return total / 3.0


def checker_sign():
    plane_ids = jnp.arange(NZ, dtype=jnp.int32)[:, None, None]
    column_ids = jnp.arange(NX, dtype=jnp.int32)[None, :, None]
    row_ids = jnp.arange(NY, dtype=jnp.int32)[None, None, :]
    parity = (plane_ids + column_ids + row_ids) % 2
    return 1.0 - 2.0 * parity.astype(jnp.float32)


def block_table(key, low, high, width):
    count = (NZ + width - 1) // width
    plane_ids = jnp.arange(NZ, dtype=jnp.int32)
    values = jax.random.uniform(key, (count,), jnp.float32, low, high)
    return values[plane_ids // width]


def mixed_field(key, salt):
    white = base_noise(jax.random.fold_in(key, salt + 1))
    smooth = box_filter(base_noise(jax.random.fold_in(key, salt + 2)))
    rough = checker_sign() * box_filter(base_noise(jax.random.fold_in(key, salt + 3)))
    mixing = block_table(jax.random.fold_in(key, salt + 4), -1.2, 1.2, 8)
    mixing = mixing + block_table(jax.random.fold_in(key, salt + 5), -0.5, 0.5, 2)
    upward = jnp.maximum(mixing, 0.0)[:, None, None]
    downward = jnp.maximum(-mixing, 0.0)[:, None, None]
    field = white + upward * smooth + downward * rough
    amplitude = jnp.exp(block_table(jax.random.fold_in(key, salt + 6), 0.0, math.log(10.0), 8))
    return (field, amplitude)


def paired_fields(key):
    depth = jnp.arange(NZ, dtype=jnp.float32) / max(NZ - 1, 1)
    direction_base, direction_amp = mixed_field(key, 100)
    residual_base, residual_amp = mixed_field(key, 200)
    coupling = block_table(jax.random.fold_in(key, 301), -1.0, 1.0, 8)
    coupling = coupling + block_table(jax.random.fold_in(key, 302), -0.3, 0.3, 2)
    trend = 3.0 ** depth
    direction = (0.2 * trend * direction_amp)[:, None, None] * direction_base
    residual = (0.2 * trend * residual_amp)[:, None, None] * (residual_base + coupling[:, None, None] * direction_base)
    return (jnp.clip(residual, -39.0, 39.0), jnp.clip(direction, -39.0, 39.0))


def draw_residual(key, part):
    return paired_fields(key)[0]


def draw_direction(key, part):
    return paired_fields(key)[1]


def shard_levels(own_key, dims, pieces, least, largest):
    factor_of = 1.0
    for dim, parts in pieces:
        steps = jax.random.uniform(jax.random.fold_in(jax.random.fold_in(own_key, 6), dim), (parts,), jnp.float32, least / len(pieces), largest / len(pieces))
        factor_of = factor_of * jnp.repeat(jnp.exp(steps), dims[dim] // parts).reshape((-1,) + (1,) * (len(dims) - 1 - dim))
    return factor_of


def scatter_about(stream_key, extent, spread, reach, cuts=(), kind=jnp.bfloat16):
    drawn = spread * jax.random.normal(stream_key, extent, jnp.float32)
    if cuts:
        drawn = drawn * shard_levels(stream_key, extent, cuts, -0.22, 0.18)
    return jnp.clip(drawn, -reach, reach).astype(kind)


def setup_inputs(seed: int = 0) -> dict:
    arg_keys = jax.random.split(jax.random.key(seed), 4)
    solution = scatter_about(arg_keys[0], (NZ, NX, NY), 1.0, 6.0, ((0, 32),), jnp.float32)
    residual = draw_residual(jax.random.fold_in(arg_keys[3], 71), 0)
    direction = draw_direction(jax.random.fold_in(arg_keys[3], 71), 0)
    return dict(solution=solution, residual=residual, direction=direction)


precise = lax.Precision.HIGHEST
first_scale = -1.0 / 6.0
next_scale = -1.0 / 3.0


def neighbours_padded(extended):
    centre = extended[:, 1:-1]
    total = extended[:, 2:] + extended[:, :-2]
    padded = jnp.pad(centre, ((0, 0), (0, 0), (1, 1), (1, 1)))
    total = total + padded[:, :, 2:, 1:-1] + padded[:, :, :-2, 1:-1]
    total = total + padded[:, :, 1:-1, 2:] + padded[:, :, 1:-1, :-2]
    return total


def change_matrix(steps):
    count = 2 * steps + 1
    table = np.zeros((count, count), np.float32)
    for offset, length in ((0, steps + 1), (steps + 1, steps)):
        for power in range(length - 1):
            column = offset + power
            table[column, column] = 6.0
            if power == 0:
                table[column + 1, column] = 6.0
            else:
                table[column + 1, column] = 3.0
                table[column - 1, column] = 3.0
    return table


def quadratic(left, gram, right):
    return jnp.dot(left, jnp.dot(gram, right, precision=precise), precision=precise)


def inner_steps(gram, steps):
    table = jnp.asarray(change_matrix(steps), jnp.float32)
    count = 2 * steps + 1
    unit_rows = jnp.eye(count, dtype=jnp.float32)
    search = unit_rows[0]
    remain = unit_rows[steps + 1]
    iterate = jnp.zeros((count,), jnp.float32)
    current = quadratic(remain, gram, remain)
    for step in range(steps):
        moved = jnp.dot(table, search, precision=precise)
        alpha = current / quadratic(search, gram, moved)
        iterate = iterate + alpha * search
        remain = remain - alpha * moved
        updated = quadratic(remain, gram, remain)
        search = remain + (updated / current) * search
        current = updated
    return jnp.stack([iterate, remain, search])


def reference(solution, residual, direction):
    current = jnp.stack([direction, residual])
    earlier = current
    search_chain = [direction]
    residual_chain = [residual]
    for power in range(1, S + 1):
        active = current if power < S else current[0:1]
        beside = neighbours_padded(jnp.pad(active, ((0, 0), (1, 1), (0, 0), (0, 0))))
        if power == 1:
            following = beside * first_scale
        else:
            following = beside * next_scale - earlier[:active.shape[0]]
        earlier = active
        current = following
        search_chain.append(following[0])
        if power < S:
            residual_chain.append(following[1])
    basis = jnp.stack(search_chain + residual_chain)
    flat = basis.reshape(basis.shape[0], -1)
    gram = jnp.dot(flat, flat.T, precision=precise, preferred_element_type=jnp.float32)
    coefs = inner_steps(gram, S)
    combined = jnp.dot(coefs, flat, precision=precise, preferred_element_type=jnp.float32)
    shape = solution.shape
    return (solution + combined[0].reshape(shape), combined[1].reshape(shape), combined[2].reshape(shape))
```

```python
import functools

import jax
import jax.numpy as jnp
import numpy as np
from jax import lax
from jax.experimental import pallas as pl
from jax.experimental.pallas import tpu as pltpu
from jax.sharding import PartitionSpec as P

S = 8
MESH = pl.DeviceIdType.MESH
first_scale = -1.0 / 6.0
next_scale = -1.0 / 3.0
SIDE = 24
LANES = 128


def change_matrix(steps):
    count = 2 * steps + 1
    table = np.zeros((count, count), np.float64)
    for offset, length in ((0, steps + 1), (steps + 1, steps)):
        for power in range(length - 1):
            column = offset + power
            table[column, column] = 6.0
            if power == 0:
                table[column + 1, column] = 6.0
            else:
                table[column + 1, column] = 3.0
                table[column - 1, column] = 3.0
    return table


def dd(power, odd):
    return 2 * power + odd


def rr(power, odd):
    return 2 * S + 1 + 2 * power + odd


def dr(power, odd):
    return 4 * S + 2 * power + odd


COUNT = 6 * S


def gram_tables():
    def moment(kind, order):
        half, odd = order // 2, order % 2
        row = np.zeros(COUNT)
        row[kind(half, odd)] += 2.0
        row[kind(0, odd)] -= 1.0
        return row

    size = 2 * S + 1
    table = np.zeros((COUNT, size, size))
    for i in range(size):
        for j in range(size):
            a, b = (i if i <= S else i - S - 1), (j if j <= S else j - S - 1)
            kind = dd if (i <= S and j <= S) else rr if (i > S and j > S) else dr
            table[:, i, j] = 0.5 * (moment(kind, a + b) + moment(kind, abs(a - b)))
    moved = table @ change_matrix(S)

    def padded(t):
        out = np.zeros((t.shape[0], SIDE, LANES), np.float32)
        out[:, :size, :size] = t
        return out

    change = np.stack([change_matrix(S), change_matrix(S).T])
    return padded(table), padded(moved), padded(change)


def kernel(gz_count, ga, sol_ref, res_ref, dir_ref, gram_tab, moved_tab, change_tab,
           out_s, out_r, out_d,
           X, halo, stage, accs, red1, red2, coef, outbuf, fin,
           in_send, in_recv, own_sem, z_send, z_recv, r_send, r_recv,
           a_send, a_recv, b_send, b_recv, o_send, o_recv):
    group = 2 * ga
    groups = gz_count // 2
    planes, width, depth = sol_ref.shape
    tall = planes * group
    rows = width // group
    iz, ia = lax.axis_index("gz"), lax.axis_index("ga")
    g = iz // 2
    p = (iz % 2) * ga + ia

    def place(position):
        upper = position // ga
        return upper * (3 * ga - 1 - position) + (1 - upper) * position

    b = place(p)

    def device(which, position):
        return (which * 2 + position // ga, position % ga)

    def block_rows(block):
        return pl.ds(pl.multiple_of(block * rows, rows), rows)

    barrier = pltpu.get_barrier_semaphore()
    for j in range(1, group):
        pl.semaphore_signal(barrier, inc=1, device_id=device(g, (p + j) % group), device_id_type=MESH)
    for j in range(1, groups):
        pl.semaphore_signal(barrier, inc=1, device_id=device((g + j) % groups, p), device_id_type=MESH)
    pl.semaphore_wait(barrier, group - 1 + groups - 1)

    sources = (dir_ref, res_ref)

    def incoming(c, j):
        q = (p + j) % group
        return pltpu.make_async_remote_copy(
            src_ref=sources[c].at[:, block_rows(place(q)), :],
            dst_ref=X.at[c, 0, pl.ds(1 + planes * p, planes)],
            send_sem=in_send.at[c, j], recv_sem=in_recv.at[c, j],
            device_id=device(g, q), device_id_type=MESH)

    def own_in(c):
        return pltpu.make_async_copy(
            sources[c].at[:, block_rows(b), :],
            X.at[c, 0, pl.ds(1 + planes * p, planes)], own_sem.at[c])

    for c in range(2):
        for j in range(1, group):
            incoming(c, j).start()
        own_in(c).start()

    below, above = g > 0, g < groups - 1
    before, after = b > 0, b < group - 1

    @pl.when(g == 0)
    def _():
        for c in range(2):
            for k in range(S):
                X[c, k, 0] = jnp.zeros((rows, depth), jnp.float32)

    @pl.when(g == groups - 1)
    def _():
        for c in range(2):
            for k in range(S):
                X[c, k, tall + 1] = jnp.zeros((rows, depth), jnp.float32)

    @pl.when(b == 0)
    def _():
        for c in range(2):
            for k in range(S):
                halo[c, k, 0] = jnp.zeros((tall, depth), jnp.float32)

    @pl.when(b == group - 1)
    def _():
        for c in range(2):
            for k in range(S):
                halo[c, k, 1] = jnp.zeros((tall, depth), jnp.float32)

    def z_copy(c, k, up):
        return pltpu.make_async_remote_copy(
            src_ref=X.at[c, k, tall if up else 1],
            dst_ref=X.at[c, k, 0 if up else tall + 1],
            send_sem=z_send.at[c, k, up], recv_sem=z_recv.at[c, k, up],
            device_id=device(g + (1 if up else -1), p), device_id_type=MESH)

    def r_copy(c, k, up):
        return pltpu.make_async_remote_copy(
            src_ref=stage.at[c, k, up],
            dst_ref=halo.at[c, k, 1 - up],
            send_sem=r_send.at[c, k, up], recv_sem=r_recv.at[c, k, up],
            device_id=device(g, place(b + (1 if up else -1))), device_id_type=MESH)

    def send_z(c, k):
        @pl.when(below)
        def _():
            z_copy(c, k, 0).start()

        @pl.when(above)
        def _():
            z_copy(c, k, 1).start()

    def send_rows(c, k):
        @pl.when(before)
        def _():
            r_copy(c, k, 0).start()

        @pl.when(after)
        def _():
            r_copy(c, k, 1).start()

    def receive(c, k):
        @pl.when(before)
        def _():
            r_copy(c, k, 1).wait_recv()

        @pl.when(after)
        def _():
            r_copy(c, k, 0).wait_recv()

        @pl.when(below)
        def _():
            z_copy(c, k, 1).wait_recv()

        @pl.when(above)
        def _():
            z_copy(c, k, 0).wait_recv()

    row_ids = lax.broadcasted_iota(jnp.int32, (rows, depth), 0)
    col_ids = lax.broadcasted_iota(jnp.int32, (rows, depth), 1)
    first_row, last_row = row_ids == 0, row_ids == rows - 1
    first_col, last_col = col_ids == 0, col_ids == depth - 1

    def folded(x):
        total = x[0:8]
        for i in range(8, rows, 8):
            total = total + x[i:i + 8]
        out = total[:, 0:LANES]
        for i in range(LANES, depth, LANES):
            out = out + total[:, i:i + LANES]
        return out

    def chain_step(c, k):
        if c == 0:
            names = [(dd(k, 0), "new", "new"), (dd(k - 1, 1), "new", "cur")]
            if k == 1:
                names.append((dd(0, 0), "cur", "cur"))
            if k == S:
                names.append((dr(S - 1, 1), "new", "other"))
        else:
            names = [(rr(k, 0), "new", "new"), (rr(k - 1, 1), "new", "cur"),
                     (dr(k, 0), "new", "other"), (dr(k - 1, 1), "cur", "other")]
            if k == 1:
                names += [(rr(0, 0), "cur", "cur"), (dr(0, 0), "cur", "start")]

        def plane(z, sums):
            cur = X[c, k - 1, z + 1]
            total = X[c, k - 1, z] + X[c, k - 1, z + 2]
            low = halo[c, k - 1, 0, pl.ds(z, 1), :]
            high = halo[c, k - 1, 1, pl.ds(z, 1), :]
            total = total + jnp.where(first_row, low, pltpu.roll(cur, 1, 0))
            total = total + jnp.where(last_row, high, pltpu.roll(cur, rows - 1, 0))
            total = total + jnp.where(first_col, 0.0, pltpu.roll(cur, 1, 1))
            total = total + jnp.where(last_col, 0.0, pltpu.roll(cur, depth - 1, 1))
            if k == 1:
                new = total * first_scale
            else:
                new = total * next_scale - X[c, k - 2, z + 1]
            X[c, k, z + 1] = new
            if k < (S if c == 0 else S - 1):
                stage[c, k, 0, pl.ds(z, 1), :] = new[0:1]
                stage[c, k, 1, pl.ds(z, 1), :] = new[rows - 1:rows]
            have = {"new": new, "cur": cur}
            if any("other" in n for n in names):
                have["other"] = X[1, S - 1, z + 1] if c == 0 else X[0, k, z + 1]
            if any("start" in n for n in names):
                have["start"] = X[0, 0, z + 1]
            return tuple(s + folded(have[l] * have[r]) for s, (_, l, r) in zip(sums, names))

        more = k < (S if c == 0 else S - 1)
        sums = tuple(jnp.zeros((8, LANES), jnp.float32) for _ in names)
        sums = plane(0, sums)
        sums = plane(tall - 1, sums)
        if more:
            send_z(c, k)
        sums = lax.fori_loop(1, tall - 1, plane, sums, unroll=2)
        if more:
            send_rows(c, k)
        for s, (slot, _, _) in zip(sums, names):
            accs[slot] = s

    def arrive(c):
        own_in(c).wait()
        for j in range(1, group):
            incoming(c, j).wait_recv()
        send_z(c, 0)
        for z in range(tall):
            stage[c, 0, 0, z:z + 1, :] = X[c, 0, z + 1, 0:1, :]
            stage[c, 0, 1, z:z + 1, :] = X[c, 0, z + 1, rows - 1:rows, :]
        send_rows(c, 0)

    arrive(0)
    receive(0, 0)
    chain_step(0, 1)
    arrive(1)
    receive(1, 0)
    chain_step(1, 1)
    for k in range(2, S + 1):
        receive(0, k - 1)
        chain_step(0, k)
        if k < S:
            receive(1, k - 1)
            chain_step(1, k)

    lanes = lax.broadcasted_iota(jnp.int32, (8, LANES), 1)
    packed = jnp.zeros((8, LANES), jnp.float32)
    for t in range(COUNT // 8):
        part = jnp.sum(jnp.sum(accs[8 * t:8 * t + 8], axis=1), axis=1, keepdims=True)
        packed = packed + jnp.where(lanes == t, part, 0.0)
    red1[p] = packed

    def first_sum(j, mine):
        q = (p + j) % group
        slot = p if mine else q
        return pltpu.make_async_remote_copy(
            src_ref=red1.at[p], dst_ref=red1.at[slot],
            send_sem=a_send.at[j], recv_sem=a_recv.at[slot],
            device_id=device(g, q), device_id_type=MESH)

    def second_sum(j, mine):
        q = (g + j) % groups
        slot = g if mine else q
        return pltpu.make_async_remote_copy(
            src_ref=red2.at[g], dst_ref=red2.at[slot],
            send_sem=b_send.at[j], recv_sem=b_recv.at[slot],
            device_id=device(q, p), device_id_type=MESH)

    for j in range(1, group):
        first_sum(j, True).start()
    for j in range(1, group):
        first_sum(j, False).wait_recv()
    total = red1[0]
    for i in range(1, group):
        total = total + red1[i]
    red2[g] = total
    for j in range(1, groups):
        second_sum(j, True).start()
    for j in range(1, groups):
        second_sum(j, False).wait_recv()
    total = red2[0]
    for i in range(1, groups):
        total = total + red2[i]

    gram = jnp.zeros((SIDE, LANES), jnp.float32)
    moved = jnp.zeros((SIDE, LANES), jnp.float32)
    for e in range(COUNT):
        value = total[e % 8:e % 8 + 1, e // 8:e // 8 + 1]
        gram = gram + value * gram_tab[e]
        moved = moved + value * moved_tab[e]
    change, change_t = change_tab[0], change_tab[1]

    def full(x):
        return jnp.sum(jnp.sum(x, axis=0, keepdims=True), axis=1, keepdims=True)

    def unit(axis, at):
        ids = lax.broadcasted_iota(jnp.int32, (SIDE, LANES), axis)
        return jnp.where(ids == at, 1.0, 0.0).astype(jnp.float32)

    def inner(_, state):
        qc, qr, wc, wr, it, rho = state
        alpha = rho / full(qc * (moved * qr))
        mc = jnp.sum(change * qr, axis=1, keepdims=True)
        mr = jnp.sum(change_t * qc, axis=0, keepdims=True)
        it = it + alpha * qc
        wc = wc - alpha * mc
        wr = wr - alpha * mr
        rho_new = full(wc * (gram * wr))
        beta = rho_new / rho
        return wc + beta * qc, wr + beta * qr, wc, wr, it, rho_new

    wc, wr = unit(0, S + 1), unit(1, S + 1)
    state = (unit(0, 0), unit(1, 0), wc, wr, jnp.zeros((SIDE, LANES), jnp.float32),
             full(wc * (gram * wr)))
    qc, qr, wc, wr, it, rho = lax.fori_loop(0, S, inner, state)
    coef[0] = it
    coef[1] = wc
    coef[2] = qc

    def outgoing(j):
        q = (p + j) % group
        return pltpu.make_async_remote_copy(
            src_ref=outbuf.at[q],
            dst_ref=fin.at[:, :, block_rows(b), :],
            send_sem=o_send.at[j], recv_sem=o_recv.at[j],
            device_id=device(g, q), device_id_type=MESH)

    def outgoing_from(j):
        q = (p + group - j) % group
        return pltpu.make_async_remote_copy(
            src_ref=outbuf.at[q],
            dst_ref=fin.at[:, :, block_rows(place(q)), :],
            send_sem=o_send.at[j], recv_sem=o_recv.at[j],
            device_id=device(g, q), device_id_type=MESH)

    def combine(q):
        for i in range(planes):
            def strip(s, carry):
                at = pl.ds(pl.multiple_of(s * 16, 16), 16)
                sums = [None, None, None]
                for v in range(2 * S + 1):
                    c, k = (0, v) if v <= S else (1, v - S - 1)
                    x = X[c, k, planes * q + i + 1, at, :]
                    for o in range(3):
                        f = coef[o, v:v + 1, :]
                        f = jnp.concatenate([f] * (depth // LANES), axis=1)
                        term = f * x
                        sums[o] = term if sums[o] is None else sums[o] + term
                for o in range(3):
                    outbuf[q, o, i, at, :] = sums[o]
                return carry
            lax.fori_loop(0, rows // 16, strip, 0)

    for j in range(1, group):
        combine((p + j) % group)
        outgoing(j).start()
    combine(p)
    own_out = pltpu.make_async_copy(outbuf.at[p], fin.at[:, :, block_rows(b), :], own_sem.at[2])
    own_out.start()
    own_out.wait()
    for j in range(1, group):
        outgoing_from(j).wait_recv()

    out_s[...] = sol_ref[...] + fin[0]
    out_r[...] = fin[1]
    out_d[...] = fin[2]

    for c in range(2):
        for j in range(1, group):
            incoming(c, j).wait_send()
        for k in range(S if c == 0 else S - 1):
            @pl.when(below)
            def _():
                z_copy(c, k, 0).wait_send()

            @pl.when(above)
            def _():
                z_copy(c, k, 1).wait_send()

            @pl.when(before)
            def _():
                r_copy(c, k, 0).wait_send()

            @pl.when(after)
            def _():
                r_copy(c, k, 1).wait_send()
    for j in range(1, group):
        first_sum(j, True).wait_send()
        outgoing(j).wait_send()
    for j in range(1, groups):
        second_sum(j, True).wait_send()


def on_device(gz_count, ga, sol, res, direction):
    planes, width, depth = sol.shape
    group, groups = 2 * ga, gz_count // 2
    tall, rows = planes * group, width // group
    gram_tab, moved_tab, change_tab = (jnp.asarray(t) for t in gram_tables())
    vmem = pl.BlockSpec(memory_space=pltpu.VMEM)
    dma = pltpu.SemaphoreType.DMA
    shape = jax.ShapeDtypeStruct(sol.shape, jnp.float32)
    f32 = jnp.float32
    return pl.pallas_call(
        functools.partial(kernel, gz_count, ga),
        out_shape=(shape, shape, shape),
        in_specs=[vmem] * 6,
        out_specs=(vmem, vmem, vmem),
        scratch_shapes=[
            pltpu.VMEM((2, S + 1, tall + 2, rows, depth), f32),
            pltpu.VMEM((2, S, 2, tall, depth), f32),
            pltpu.VMEM((2, S, 2, tall, depth), f32),
            pltpu.VMEM((COUNT, 8, LANES), f32),
            pltpu.VMEM((group, 8, LANES), f32),
            pltpu.VMEM((groups, 8, LANES), f32),
            pltpu.VMEM((3, SIDE, LANES), f32),
            pltpu.VMEM((group, 3, planes, rows, depth), f32),
            pltpu.VMEM((3, planes, width, depth), f32),
            dma((2, group)), dma((2, group)), dma((3,)),
            dma((2, S, 2)), dma((2, S, 2)), dma((2, S, 2)), dma((2, S, 2)),
            dma((group,)), dma((group,)), dma((groups,)), dma((groups,)),
            dma((group,)), dma((group,)),
        ],
        compiler_params=pltpu.CompilerParams(collective_id=0, has_side_effects=True),
    )(sol, res, direction, gram_tab, moved_tab, change_tab)


def solution(mesh):
    spec = P(("gz", "ga"), None, None)
    return jax.shard_map(
        functools.partial(on_device, mesh.shape["gz"], mesh.shape["ga"]),
        mesh=mesh, in_specs=(spec, spec, spec), out_specs=(spec, spec, spec), check_vma=False,
    )
```

```python
import functools

import jax
import jax.numpy as jnp
import numpy as np
from jax import lax
from jax.experimental import pallas as pl
from jax.experimental.pallas import tpu as pltpu
from jax.sharding import PartitionSpec as P

S = 8
MESH = pl.DeviceIdType.MESH
first_scale = -1.0 / 6.0
next_scale = -1.0 / 3.0
SIDE = 24
LANES = 128


def change_matrix(steps):
    count = 2 * steps + 1
    table = np.zeros((count, count), np.float64)
    for offset, length in ((0, steps + 1), (steps + 1, steps)):
        for power in range(length - 1):
            column = offset + power
            table[column, column] = 6.0
            if power == 0:
                table[column + 1, column] = 6.0
            else:
                table[column + 1, column] = 3.0
                table[column - 1, column] = 3.0
    return table


def dd(power, odd):
    return 2 * power + odd


def rr(power, odd):
    return 2 * S + 1 + 2 * power + odd


def dr(power, odd):
    return 4 * S + 2 * power + odd


COUNT = 6 * S


def gram_tables():
    def moment(kind, order):
        half, odd = order // 2, order % 2
        row = np.zeros(COUNT)
        row[kind(half, odd)] += 2.0
        row[kind(0, odd)] -= 1.0
        return row

    size = 2 * S + 1
    table = np.zeros((COUNT, size, size))
    for i in range(size):
        for j in range(size):
            a, b = (i if i <= S else i - S - 1), (j if j <= S else j - S - 1)
            kind = dd if (i <= S and j <= S) else rr if (i > S and j > S) else dr
            table[:, i, j] = 0.5 * (moment(kind, a + b) + moment(kind, abs(a - b)))
    moved = table @ change_matrix(S)

    def padded(t):
        out = np.zeros((t.shape[0], SIDE, LANES), np.float32)
        out[:, :size, :size] = t
        return out

    change = np.stack([change_matrix(S), change_matrix(S).T])
    return padded(table), padded(moved), padded(change)


def kernel(gz_count, ga, res_ref, dir_ref, gram_hbm, moved_hbm, change_tab,
           fin,
           X, halo, stage, accs, red1, red2, coef, outbuf, held, gram_tab, moved_tab,
           in_send, in_recv, own_sem, z_send, z_recv, r_send, r_recv,
           a_send, a_recv, b_send, b_recv, o_send, o_recv, load_sem):
    group = 2 * ga
    groups = gz_count // 2
    planes, width, depth = res_ref.shape
    tall = planes * group
    rows = width // group
    iz, ia = lax.axis_index("gz"), lax.axis_index("ga")
    g = iz // 2
    p = (iz % 2) * ga + ia

    def place(position):
        upper = position // ga
        return upper * (3 * ga - 1 - position) + (1 - upper) * position

    b = place(p)

    def device(which, position):
        return (which * 2 + position // ga, position % ga)

    def block_rows(block):
        return pl.ds(pl.multiple_of(block * rows, rows), rows)

    loads = [pltpu.make_async_copy(source, target, load_sem.at[i]) for i, (source, target) in enumerate((
        (dir_ref, held.at[0]), (res_ref, held.at[1]), (gram_hbm, gram_tab), (moved_hbm, moved_tab)))]
    for load in loads:
        load.start()

    barrier = pltpu.get_barrier_semaphore()
    for j in range(1, group):
        pl.semaphore_signal(barrier, inc=1, device_id=device(g, (p + j) % group), device_id_type=MESH)
    for j in range(1, groups):
        pl.semaphore_signal(barrier, inc=1, device_id=device((g + j) % groups, p), device_id_type=MESH)
    pl.semaphore_wait(barrier, group - 1 + groups - 1)

    def incoming(c, j):
        q = (p + j) % group
        return pltpu.make_async_remote_copy(
            src_ref=held.at[c, :, block_rows(place(q)), :],
            dst_ref=X.at[c, 0, pl.ds(1 + planes * p, planes)],
            send_sem=in_send.at[c, j], recv_sem=in_recv.at[c, j],
            device_id=device(g, q), device_id_type=MESH)

    def own_in(c):
        return pltpu.make_async_copy(
            held.at[c, :, block_rows(b), :],
            X.at[c, 0, pl.ds(1 + planes * p, planes)], own_sem.at[c])

    for c in range(2):
        loads[c].wait()
        for j in range(1, group):
            incoming(c, j).start()
        own_in(c).start()

    below, above = g > 0, g < groups - 1
    before, after = b > 0, b < group - 1

    @pl.when(g == 0)
    def _():
        for c in range(2):
            for k in range(S):
                X[c, k, 0] = jnp.zeros((rows, depth), jnp.float32)

    @pl.when(g == groups - 1)
    def _():
        for c in range(2):
            for k in range(S):
                X[c, k, tall + 1] = jnp.zeros((rows, depth), jnp.float32)

    @pl.when(b == 0)
    def _():
        for c in range(2):
            for k in range(S):
                halo[c, k, 0] = jnp.zeros((tall, depth), jnp.float32)

    @pl.when(b == group - 1)
    def _():
        for c in range(2):
            for k in range(S):
                halo[c, k, 1] = jnp.zeros((tall, depth), jnp.float32)

    def z_copy(c, k, up):
        return pltpu.make_async_remote_copy(
            src_ref=X.at[c, k, tall if up else 1],
            dst_ref=X.at[c, k, 0 if up else tall + 1],
            send_sem=z_send.at[c, k, up], recv_sem=z_recv.at[c, k, up],
            device_id=device(g + (1 if up else -1), p), device_id_type=MESH)

    def r_copy(c, k, up):
        return pltpu.make_async_remote_copy(
            src_ref=stage.at[c, k, up],
            dst_ref=halo.at[c, k, 1 - up],
            send_sem=r_send.at[c, k, up], recv_sem=r_recv.at[c, k, up],
            device_id=device(g, place(b + (1 if up else -1))), device_id_type=MESH)

    def send_z(c, k):
        @pl.when(below)
        def _():
            z_copy(c, k, 0).start()

        @pl.when(above)
        def _():
            z_copy(c, k, 1).start()

    def send_rows(c, k):
        @pl.when(before)
        def _():
            r_copy(c, k, 0).start()

        @pl.when(after)
        def _():
            r_copy(c, k, 1).start()

    def receive(c, k):
        @pl.when(before)
        def _():
            r_copy(c, k, 1).wait_recv()

        @pl.when(after)
        def _():
            r_copy(c, k, 0).wait_recv()

        @pl.when(below)
        def _():
            z_copy(c, k, 1).wait_recv()

        @pl.when(above)
        def _():
            z_copy(c, k, 0).wait_recv()

    row_ids = lax.broadcasted_iota(jnp.int32, (rows, depth), 0)
    col_ids = lax.broadcasted_iota(jnp.int32, (rows, depth), 1)
    first_row, last_row = row_ids == 0, row_ids == rows - 1
    first_col, last_col = col_ids == 0, col_ids == depth - 1

    def folded(x):
        total = x[0:8]
        for i in range(8, rows, 8):
            total = total + x[i:i + 8]
        out = total[:, 0:LANES]
        for i in range(LANES, depth, LANES):
            out = out + total[:, i:i + LANES]
        return out

    def chain_step(c, k):
        if c == 0:
            names = [(dd(k, 0), "new", "new"), (dd(k - 1, 1), "new", "cur")]
            if k == 1:
                names.append((dd(0, 0), "cur", "cur"))
        else:
            names = [(rr(k, 0), "new", "new"), (rr(k - 1, 1), "new", "cur"),
                     (dr(k, 0), "new", "other"), (dr(k - 1, 1), "cur", "other")]
            if k == S - 1:
                names.append((dr(k, 1), "new", "ahead"))
            if k == 1:
                names += [(rr(0, 0), "cur", "cur"), (dr(0, 0), "cur", "start")]

        def plane(z, sums):
            cur = X[c, k - 1, z + 1]
            total = X[c, k - 1, z] + X[c, k - 1, z + 2]
            low = halo[c, k - 1, 0, pl.ds(z, 1), :]
            high = halo[c, k - 1, 1, pl.ds(z, 1), :]
            total = total + jnp.where(first_row, low, pltpu.roll(cur, 1, 0))
            total = total + jnp.where(last_row, high, pltpu.roll(cur, rows - 1, 0))
            total = total + jnp.where(first_col, 0.0, pltpu.roll(cur, 1, 1))
            total = total + jnp.where(last_col, 0.0, pltpu.roll(cur, depth - 1, 1))
            if k == 1:
                new = total * first_scale
            else:
                new = total * next_scale - X[c, k - 2, z + 1]
            X[c, k, z + 1] = new
            if k < (S if c == 0 else S - 1):
                stage[c, k, 0, pl.ds(z, 1), :] = new[0:1]
                stage[c, k, 1, pl.ds(z, 1), :] = new[rows - 1:rows]
            have = {"new": new, "cur": cur}
            if any("other" in n for n in names):
                have["other"] = X[0, k, z + 1]
            if any("ahead" in n for n in names):
                have["ahead"] = X[0, k + 1, z + 1]
            if any("start" in n for n in names):
                have["start"] = X[0, 0, z + 1]
            return tuple(s + folded(have[l] * have[r]) for s, (_, l, r) in zip(sums, names))

        more = k < (S if c == 0 else S - 1)
        sums = tuple(jnp.zeros((8, LANES), jnp.float32) for _ in names)
        sums = plane(0, sums)
        sums = plane(tall - 1, sums)
        if more:
            send_z(c, k)
        sums = lax.fori_loop(1, tall - 1, plane, sums, unroll=7)
        if more:
            send_rows(c, k)
        for s, (slot, _, _) in zip(sums, names):
            accs[slot] = s

    def arrive(c):
        own_in(c).wait()
        for j in range(1, group):
            incoming(c, j).wait_recv()
        send_z(c, 0)
        for z in range(tall):
            stage[c, 0, 0, z:z + 1, :] = X[c, 0, z + 1, 0:1, :]
            stage[c, 0, 1, z:z + 1, :] = X[c, 0, z + 1, rows - 1:rows, :]
        send_rows(c, 0)

    arrive(0)
    receive(0, 0)
    chain_step(0, 1)
    receive(0, 1)
    chain_step(0, 2)
    arrive(1)
    for k in range(1, S):
        receive(1, k - 1)
        chain_step(1, k)
        if k + 2 <= S:
            receive(0, k + 1)
            chain_step(0, k + 2)

    lanes = lax.broadcasted_iota(jnp.int32, (8, LANES), 1)
    packed = jnp.zeros((8, LANES), jnp.float32)
    for t in range(COUNT // 8):
        part = jnp.sum(jnp.sum(accs[8 * t:8 * t + 8], axis=1), axis=1, keepdims=True)
        packed = packed + jnp.where(lanes == t, part, 0.0)
    red1[p] = packed

    def first_sum(j, mine):
        q = (p + j) % group
        slot = p if mine else q
        return pltpu.make_async_remote_copy(
            src_ref=red1.at[p], dst_ref=red1.at[slot],
            send_sem=a_send.at[j], recv_sem=a_recv.at[slot],
            device_id=device(g, q), device_id_type=MESH)

    def second_sum(j, mine):
        q = (g + j) % groups
        slot = g if mine else q
        return pltpu.make_async_remote_copy(
            src_ref=red2.at[g], dst_ref=red2.at[slot],
            send_sem=b_send.at[j], recv_sem=b_recv.at[slot],
            device_id=device(q, p), device_id_type=MESH)

    for j in range(1, group):
        first_sum(j, True).start()
    for j in range(1, group):
        first_sum(j, False).wait_recv()
    total = red1[0]
    for i in range(1, group):
        total = total + red1[i]
    red2[g] = total
    for j in range(1, groups):
        second_sum(j, True).start()
    for j in range(1, groups):
        second_sum(j, False).wait_recv()
    total = red2[0]
    for i in range(1, groups):
        total = total + red2[i]

    loads[2].wait()
    loads[3].wait()
    gram = jnp.zeros((SIDE, LANES), jnp.float32)
    moved = jnp.zeros((SIDE, LANES), jnp.float32)
    for e in range(COUNT):
        value = total[e % 8:e % 8 + 1, e // 8:e // 8 + 1]
        gram = gram + value * gram_tab[e]
        moved = moved + value * moved_tab[e]
    change, change_t = change_tab[0], change_tab[1]

    def full(x):
        return jnp.sum(jnp.sum(x, axis=0, keepdims=True), axis=1, keepdims=True)

    def unit(axis, at):
        ids = lax.broadcasted_iota(jnp.int32, (SIDE, LANES), axis)
        return jnp.where(ids == at, 1.0, 0.0).astype(jnp.float32)

    def inner(_, state):
        qc, qr, wc, wr, it, rho = state
        alpha = rho / full(qc * (moved * qr))
        mc = jnp.sum(change * qr, axis=1, keepdims=True)
        mr = jnp.sum(change_t * qc, axis=0, keepdims=True)
        it = it + alpha * qc
        wc = wc - alpha * mc
        wr = wr - alpha * mr
        rho_new = full(wc * (gram * wr))
        beta = rho_new / rho
        return wc + beta * qc, wr + beta * qr, wc, wr, it, rho_new

    wc, wr = unit(0, S + 1), unit(1, S + 1)
    state = (unit(0, 0), unit(1, 0), wc, wr, jnp.zeros((SIDE, LANES), jnp.float32),
             full(wc * (gram * wr)))
    qc, qr, wc, wr, it, rho = lax.fori_loop(0, S, inner, state)
    coef[0] = it
    coef[1] = wc
    coef[2] = qc

    def outgoing(j):
        q = (p + j) % group
        return pltpu.make_async_remote_copy(
            src_ref=outbuf.at[q],
            dst_ref=fin.at[:, :, block_rows(b), :],
            send_sem=o_send.at[j], recv_sem=o_recv.at[j],
            device_id=device(g, q), device_id_type=MESH)

    def outgoing_from(j):
        q = (p + group - j) % group
        return pltpu.make_async_remote_copy(
            src_ref=outbuf.at[q],
            dst_ref=fin.at[:, :, block_rows(place(q)), :],
            send_sem=o_send.at[j], recv_sem=o_recv.at[j],
            device_id=device(g, q), device_id_type=MESH)

    def combine(q):
        for i in range(planes):
            def strip(s, carry):
                at = pl.ds(pl.multiple_of(s * 16, 16), 16)
                sums = [None, None, None]
                for v in range(2 * S + 1):
                    c, k = (0, v) if v <= S else (1, v - S - 1)
                    x = X[c, k, planes * q + i + 1, at, :]
                    for o in range(3):
                        f = coef[o, v:v + 1, :]
                        f = jnp.concatenate([f] * (depth // LANES), axis=1)
                        term = f * x
                        sums[o] = term if sums[o] is None else sums[o] + term
                for o in range(3):
                    outbuf[q, o, i, at, :] = sums[o]
                return carry
            lax.fori_loop(0, rows // 16, strip, 0)

    for j in range(1, group):
        combine((p + j) % group)
        outgoing(j).start()
    combine(p)
    own_out = pltpu.make_async_copy(outbuf.at[p], fin.at[:, :, block_rows(b), :], own_sem.at[2])
    own_out.start()
    own_out.wait()
    for j in range(1, group):
        outgoing_from(j).wait_recv()

    for c in range(2):
        for j in range(1, group):
            incoming(c, j).wait_send()
        for k in range(S if c == 0 else S - 1):
            @pl.when(below)
            def _():
                z_copy(c, k, 0).wait_send()

            @pl.when(above)
            def _():
                z_copy(c, k, 1).wait_send()

            @pl.when(before)
            def _():
                r_copy(c, k, 0).wait_send()

            @pl.when(after)
            def _():
                r_copy(c, k, 1).wait_send()
    for j in range(1, group):
        first_sum(j, True).wait_send()
        outgoing(j).wait_send()
    for j in range(1, groups):
        second_sum(j, True).wait_send()


def on_device(gz_count, ga, sol, res, direction):
    planes, width, depth = sol.shape
    group, groups = 2 * ga, gz_count // 2
    tall, rows = planes * group, width // group
    gram_tab, moved_tab, change_tab = (jnp.asarray(t) for t in gram_tables())
    vmem = pl.BlockSpec(memory_space=pltpu.VMEM)
    dma = pltpu.SemaphoreType.DMA
    shape = jax.ShapeDtypeStruct((3,) + sol.shape, jnp.float32)
    anywhere = pl.BlockSpec(memory_space=pl.ANY)
    f32 = jnp.float32
    combined = pl.pallas_call(
        functools.partial(kernel, gz_count, ga),
        out_shape=shape,
        in_specs=[anywhere] * 4 + [vmem],
        out_specs=vmem,
        scratch_shapes=[
            pltpu.VMEM((2, S + 1, tall + 2, rows, depth), f32),
            pltpu.VMEM((2, S, 2, tall, depth), f32),
            pltpu.VMEM((2, S, 2, tall, depth), f32),
            pltpu.VMEM((COUNT, 8, LANES), f32),
            pltpu.VMEM((group, 8, LANES), f32),
            pltpu.VMEM((groups, 8, LANES), f32),
            pltpu.VMEM((3, SIDE, LANES), f32),
            pltpu.VMEM((group, 3, planes, rows, depth), f32),
            pltpu.VMEM((2, planes, width, depth), f32),
            pltpu.VMEM((COUNT, SIDE, LANES), f32),
            pltpu.VMEM((COUNT, SIDE, LANES), f32),
            dma((2, group)), dma((2, group)), dma((3,)),
            dma((2, S, 2)), dma((2, S, 2)), dma((2, S, 2)), dma((2, S, 2)),
            dma((group,)), dma((group,)), dma((groups,)), dma((groups,)),
            dma((group,)), dma((group,)), dma((4,)),
        ],
        compiler_params=pltpu.CompilerParams(collective_id=0, has_side_effects=True),
    )(res, direction, gram_tab, moved_tab, change_tab)
    return sol + combined[0], combined[1], combined[2]


def solution(mesh):
    spec = P(("gz", "ga"), None, None)
    return jax.shard_map(
        functools.partial(on_device, mesh.shape["gz"], mesh.shape["ga"]),
        mesh=mesh, in_specs=(spec, spec, spec), out_specs=(spec, spec, spec), check_vma=False,
    )
```
